32 devices in a mesh: rep: 2 (over z, core), dp: 16 (over x, y).
Axes of the slice: x: 4, y: 4, z: 1, core: 2. Of those that a mesh axis runs over, the one named last changes fastest.
The devices are a block of a 4x4x8 slice.
Arguments:
- x: bfloat16 [32, 4096, 896], P(('rep', 'dp')), parts along dimension 0
- dy: bfloat16 [32, 4096, 896], P(('rep', 'dp')), parts along dimension 0
- w_gate: bfloat16 [2, 896, 2560], P(None, 'dp')
- w_up: bfloat16 [2, 896, 2560], P(None, 'dp')
- w_down: bfloat16 [2, 2560, 896], P(None, 'dp')
Outputs:
- output 1: bfloat16 [32, 4096, 896], P(('rep', 'dp')), parts along dimension 0
- output 2: bfloat16 [4, 896, 2560], P('rep', 'dp'), parts along dimension 0
- output 3: bfloat16 [4, 896, 2560], P('rep', 'dp'), parts along dimension 0
- output 4: bfloat16 [4, 2560, 896], P('rep', 'dp'), parts along dimension 0
There are 2 independent parts. The reference program is written for one: setup_inputs(seed, part) draws one part's arguments, and reference() takes and returns one part's arrays. A program takes and returns all parts, laid end to end along the dimension named above; an argument that names none is the same for every part.
All inputs are finite; a program needn't handle non-finite values.
Results may differ from the reference program's by a relative error of at most 0.018.
Values are sent between devices in bfloat16 or wider.
A program may use at most 768 MiB of HBM per device.

```python
import jax
import jax.numpy as jnp
from jax import lax

SEQUENCES = 16
TOKENS = 4096
D = 896
FF = 2560
LAYERS = 2
NAMES = ("w_gate", "w_up", "w_down")
SHAPES = {"w_gate": (LAYERS, D, FF), "w_up": (LAYERS, D, FF), "w_down": (LAYERS, FF, D)}


def bump(key, n, height):
    away = (jnp.arange(n, dtype=jnp.int32) - jax.random.randint(key, (), 0, n, jnp.int32)) % n
    return jnp.where(away < n // 8, height, 1.0)


def together(key, own, strength):
    shared = jax.random.normal(key, own.shape[1:], jnp.float32)
    return (own + strength * shared) * lax.rsqrt(1 + strength * strength)


def setup_inputs(seed: int = 0, part: int = 0) -> dict:
    kx, kdy, ka, kb, kz, kf, kh, kl, *kw = jax.random.split(jax.random.key(seed), 8 + len(NAMES))
    kx, kdy, ka, kb = (jax.random.fold_in(k, part) for k in (kx, kdy, ka, kb))
    shape = (SEQUENCES, TOKENS, D)
    much_x, much_dy = jax.random.uniform(kz, (2,), jnp.float32, 0.0, 1.0)
    layers = 2.0 ** jax.random.uniform(kl, (LAYERS, 1, 1), jnp.float32, -1.0, 1.0)
    x = together(ka, jax.random.normal(kx, shape, jnp.float32), much_x) * bump(kf, D, 4.0)
    dy = together(kb, jax.random.normal(kdy, shape, jnp.float32), much_dy)
    drawn = {"x": x.astype(jnp.bfloat16), "dy": (dy * (SEQUENCES * TOKENS) ** -0.5).astype(jnp.bfloat16)}
    for key, name in zip(kw, NAMES, strict=True):
        w = jax.random.normal(key, SHAPES[name], jnp.float32) * SHAPES[name][1] ** -0.5
        drawn[name] = (w * {"w_gate": 1.0, "w_up": bump(kh, FF, 4.0), "w_down": layers}[name]).astype(jnp.bfloat16)
    return drawn


def matmul(a, w):
    return jnp.dot(a, w, preferred_element_type=jnp.float32).astype(jnp.bfloat16)


def normed(h):
    wide = h.astype(jnp.float32)
    scale = lax.rsqrt(jnp.mean(wide**2, -1, keepdims=True) + 1e-6)
    return (wide * scale).astype(jnp.bfloat16)


def layer(h, w):
    a = normed(h)
    gate = jnp.dot(a, w["w_gate"], preferred_element_type=jnp.float32)
    up = jnp.dot(a, w["w_up"], preferred_element_type=jnp.float32)
    return h + matmul((jax.nn.silu(gate) * up).astype(jnp.bfloat16), w["w_down"])


def stack(weights, h):
    return lax.scan(lambda h, w: (layer(h, w), None), h, weights)[0]


def reference(x, dy, w_gate, w_up, w_down):
    weights = dict(zip(NAMES, (w_gate, w_up, w_down), strict=True))

    def take(so_far, sequence):
        h, by_y = sequence
        _, back = jax.vjp(stack, weights, h)
        by_weights, by_h = back(by_y)
        return jax.tree.map(lambda total, term: total + term.astype(jnp.float32), so_far, by_weights), by_h

    none_yet = {name: jnp.zeros(w.shape, jnp.float32) for name, w in weights.items()}
    by_weights, by_x = lax.scan(take, none_yet, (x, dy))
    return (by_x, *(by_weights[name].astype(jnp.bfloat16) for name in NAMES))
```

```python
import functools
import math

import jax
import jax.numpy as jnp
from jax import lax
from jax.experimental import pallas as pl
from jax.experimental.pallas import tpu as pltpu
from jax.sharding import PartitionSpec as P

F32, BF16 = jnp.float32, jnp.bfloat16
TILE = 512
PIECE = 512
CHUNK = 1280
VMEM = 63 * 1024 * 1024
NT = (((1,), (1,)), ((), ()))


def dot(a, b):
    return jnp.dot(a, b, preferred_element_type=F32)


def dot_nt(a, b):
    return lax.dot_general(a, b, NT, preferred_element_type=F32)


def norm_scale(wide):
    return lax.rsqrt(jnp.mean(wide**2, -1, keepdims=True) + 1e-6)


def normed(h):
    wide = h.astype(F32)
    return (wide * norm_scale(wide)).astype(BF16)


def backward_of_norm(h, by_a):
    wide = h.astype(F32)
    scale = norm_scale(wide)
    inner = jnp.mean(by_a * wide, -1, keepdims=True)
    return scale * by_a - wide * (scale**3 * inner)


def pieces(n):
    return [pl.ds(start, CHUNK) for start in range(0, n, CHUNK)]


def gated(gate, up, by_act):
    sig = jax.nn.sigmoid(gate)
    silu = gate * sig
    by_up = by_act * silu
    by_gate = by_act * up * (sig * (1.0 + gate * (1.0 - sig)))
    return (silu * up).astype(BF16), by_gate.astype(BF16), by_up.astype(BF16)


def forward_kernel(side, x_ref, wg_ref, wu_ref, wd_ref, *refs):
    shards, (gate_ref, up_ref, h_ref), outs, scratch = refs[:3], refs[3:6], refs[6:9], refs[9:]
    gather = Gather(side, 1, shards, outs, scratch)
    for number, when in enumerate((0, 1, 2, 5)):

        @pl.when(pl.program_id(0) == when)
        def _(number=number):
            gather.stage(number)

    a = normed(x_ref[...])
    total = None
    for at in pieces(wg_ref.shape[1]):
        gate, up = dot(a, wg_ref[:, at]), dot(a, wu_ref[:, at])
        gate_ref[:, at] = gate
        up_ref[:, at] = up
        act = (gate * jax.nn.sigmoid(gate) * up).astype(BF16)
        term = dot(act, wd_ref[at, :])
        total = term if total is None else total + term
    h_ref[...] = x_ref[...] + total.astype(BF16)

    @pl.when(pl.program_id(0) == pl.num_programs(0) - 1)
    def _():
        gather.stage(Gather.STAGES - 1)


def add_down(first, at, acc_ref, by_h_t, act):
    term = dot(by_h_t, act)

    @pl.when(first)
    def _():
        acc_ref[:, at] = term

    @pl.when(jnp.logical_not(first))
    def _():
        acc_ref[:, at] += term


def close_down(acc_ref, by_wd_ref):
    @pl.when(pl.program_id(0) == pl.num_programs(0) - 1)
    def _():
        for at in pieces(acc_ref.shape[1]):
            by_wd_ref[at, :] = acc_ref[:, at].T.astype(BF16)


def turn_kernel(h_ref, by_h_ref, wg_ref, wu_ref, wd_ref, by_gate_ref, by_up_ref, by_wd_ref, acc_ref):
    first = pl.program_id(0) == 0
    a, by_h = normed(h_ref[...]), by_h_ref[...]
    by_h_t = by_h.T
    for at in pieces(wg_ref.shape[1]):
        gate, up = dot(a, wg_ref[:, at]), dot(a, wu_ref[:, at])
        by_act = dot_nt(by_h, wd_ref[at, :]).astype(BF16).astype(F32)
        act, by_gate_ref[:, at], by_up_ref[:, at] = gated(gate, up, by_act)
        add_down(first, at, acc_ref, by_h_t, act)
    close_down(acc_ref, by_wd_ref)


def back_kernel(gate_ref, up_ref, by_h_ref, wd_ref, by_gate_ref, by_up_ref, by_wd_ref, acc_ref):
    first = pl.program_id(0) == 0
    by_h = by_h_ref[...]
    by_h_t = by_h.T
    for at in pieces(wd_ref.shape[0]):
        by_act = dot_nt(by_h, wd_ref[at, :]).astype(BF16).astype(F32)
        act, by_gate_ref[:, at], by_up_ref[:, at] = gated(gate_ref[:, at], up_ref[:, at], by_act)
        add_down(first, at, acc_ref, by_h_t, act)
    close_down(acc_ref, by_wd_ref)


def cut_of(rows):
    return -(-rows // 32) * 16


class Reduction:
    STAGES = 5

    @staticmethod
    def scratch(side, rows, columns):
        shapes = []
        for n in (cut_of(rows), rows - cut_of(rows)):
            shapes += [
                pltpu.VMEM((2, side // 2, n, columns), BF16),
                pltpu.VMEM((2, side // 2, n, columns), BF16),
                pltpu.VMEM((2, side // 2, n, columns), BF16),
                pltpu.VMEM((side, n, columns), BF16),
                pltpu.VMEM((2, side, n, columns), BF16),
                pltpu.VMEM((side, n, columns), F32),
                pltpu.VMEM((n, columns), BF16),
                pltpu.VMEM((2, n, columns), BF16),
                pltpu.VMEM((2, n, columns), BF16),
                pltpu.VMEM((2, n, columns), BF16),
            ]
        return [*shapes, pltpu.SemaphoreType.DMA((2, 12)), pltpu.SemaphoreType.DMA((2, 12)), pltpu.SemaphoreType.DMA((2, 3))]

    def __init__(self, side, t_ref, out_ref, scratch):
        self.side, self.t_ref, self.out_ref = side, t_ref, out_ref
        self.held = scratch[:10], scratch[10:20]
        self.send_sem, self.recv_sem, self.own_sem = scratch[20:]
        me = lax.axis_index("dp")
        self.at = me // side, me % side
        rows, columns = out_ref.shape
        cut = cut_of(rows)
        self.rows = pl.ds(0, cut), pl.ds(cut, rows - cut)
        width = -(-columns // 256) * 128
        self.columns = pl.ds(0, width), pl.ds(width, columns - width)
        self.halves = pl.ds(0, side // 2), pl.ds(side // 2, side - side // 2)

    def beside(self, axis, by):
        x, y = self.at
        side = self.side
        return ((x + by) % side) * side + y if axis == 0 else x * side + (y + by) % side

    def line(self, item, by, which):
        at = (self.at[item] + by) % self.side
        part = pl.ds(0, self.side) if which is None else self.halves[which]
        return self.t_ref.at[at, part, self.rows[item]] if item == 0 else self.t_ref.at[part, at, self.rows[item]]

    def own(self, item, number):
        _, own, _, mine, *_ = self.held[item]
        src, dst = (
            (self.line(item, 1, 0), own.at[0]),
            (self.line(item, -1 % self.side, 1), own.at[1]),
            (self.line(item, 0, None), mine),
        )[number]
        return pltpu.make_async_copy(src, dst, self.own_sem.at[item, number])

    def copy(self, item, number):
        passing, _, sums, _, near, _, far, far_in, last, last_in = self.held[item]
        first, second, back = item, 1 - item, self.side - 1
        low, high = self.halves
        left, right = self.columns
        src, dst, axis, by = (
            lambda: (self.line(item, self.side // 2, 0), passing.at[0], first, 1),
            lambda: (self.line(item, self.side // 2, 1), passing.at[1], first, back),
            lambda: (self.line(item, 1, 1), near.at[0, high], first, 1),
            lambda: (self.line(item, back, 0), near.at[1, low], first, back),
            lambda: (sums.at[0], near.at[0, low], first, 1),
            lambda: (sums.at[1], near.at[1, high], first, back),
            lambda: (far.at[:, left], far_in.at[0, :, left], second, 1),
            lambda: (far.at[:, right], far_in.at[1, :, right], second, back),
            lambda: (last.at[0, :, right], last_in.at[0, :, right], second, 1),
            lambda: (last.at[1, :, left], last_in.at[1, :, left], second, back),
            lambda: (last.at[0, :, left], last_in.at[0, :, left], second, 1),
            lambda: (last.at[1, :, right], last_in.at[1, :, right], second, back),
        )[number]()
        return pltpu.make_async_remote_copy(
            src_ref=src,
            dst_ref=dst,
            send_sem=self.send_sem.at[item, number],
            recv_sem=self.recv_sem.at[item, number],
            device_id={"dp": self.beside(axis, by)},
            device_id_type=MESH,
        )

    def start_direct(self):
        for k in (2, 3):
            for item in range(2):
                self.copy(item, k).start()

    def stage(self, number, greet=True):
        side = self.side
        if number == 0 and greet:
            barrier = pltpu.get_barrier_semaphore()
            for axis in range(2):
                for by in (1, side - 1):
                    pl.semaphore_signal(barrier, inc=1, device_id={"dp": self.beside(axis, by)}, device_id_type=MESH)
            pl.semaphore_wait(barrier, 4)
        if number == 0:
            for k in range(2):
                for item in range(2):
                    self.copy(item, k).start()
            for k in range(3):
                for item in range(2):
                    self.own(item, k).start()
        for item in range(2):
            passing, own, sums, mine, near, total, far, far_in, last, last_in = self.held[item]
            at = self.at[1 - item]
            ahead, behind, opposite = (at + 1) % side, (at + side - 1) % side, (at + side // 2) % side
            left, right = self.columns
            if number == 1:
                for way in range(2):
                    self.own(item, way).wait()
                    self.copy(item, way).wait_recv()
                    sums[way] = (passing[way].astype(F32) + own[way].astype(F32)).astype(BF16)
                    self.copy(item, 4 + way).start()
            if number == 2:
                self.own(item, 2).wait()
                for k in range(2, 6):
                    self.copy(item, k).wait_recv()
                for j in range(side):
                    total[j] = mine[j].astype(F32) + near[0, j].astype(F32) + near[1, j].astype(F32)
                far[...] = total[opposite].astype(BF16)
                last[0, :, right] = total[ahead, :, right].astype(BF16)
                last[1, :, left] = total[behind, :, left].astype(BF16)
                for k in range(6, 10):
                    self.copy(item, k).start()
            if number == 3:
                for way, place, part in ((0, ahead, left), (1, behind, right)):
                    self.copy(item, 6 + way).wait_recv()
                    last[way, :, part] = (total[place, :, part] + far_in[way, :, part].astype(F32)).astype(BF16)
                    self.copy(item, 10 + way).start()
            if number == 4:
                for k in range(8, 12):
                    self.copy(item, k).wait_recv()
                whole_sum = total[at] + last_in[0].astype(F32) + last_in[1].astype(F32)
                self.out_ref[self.rows[item], :] = whole_sum.astype(BF16)
                for k in range(12):
                    self.copy(item, k).wait_send()


def run_stages(reductions, when):
    for number in range(Reduction.STAGES - 1):

        @pl.when(pl.program_id(0) == when[number])
        def _(number=number):
            for n, reduction in enumerate(reductions):
                reduction.stage(number, greet=n == 0)
            if number == 0:
                for reduction in reductions:
                    reduction.start_direct()


def last_stage(reductions):
    @pl.when(pl.program_id(0) == pl.num_programs(0) - 1)
    def _():
        for reduction in reductions:
            reduction.stage(Reduction.STAGES - 1)


def weight_kernel(side, h_ref, by_gate_ref, by_up_ref, t_ref, gate_ref, up_ref, sum_ref, a_t_ref, *scratch):
    reductions = [Reduction(side, t_ref, sum_ref, scratch)]
    run_stages(reductions, (0, 2, 4, 6))
    half = pl.num_programs(0) // 2

    @pl.when(pl.program_id(0) == 0)
    def _():
        @pl.loop(0, h_ref.shape[0] // TILE)
        def _(i):
            at = pl.ds(pl.multiple_of(i * TILE, TILE), TILE)
            a_t_ref[:, at] = normed(h_ref[at, :]).T

    @pl.when(pl.program_id(0) < half)
    def _():
        gate_ref[...] = dot(a_t_ref[...], by_gate_ref[...]).astype(BF16)

    @pl.when(pl.program_id(0) >= half)
    def _():
        up_ref[...] = dot(a_t_ref[...], by_up_ref[...]).astype(BF16)

    last_stage(reductions)


def input_kernel(side, h_ref, by_h_ref, by_gate_ref, by_up_ref, wg_ref, wu_ref, t0_ref, t1_ref, out_ref, sum0_ref, sum1_ref, *scratch):
    count = len(scratch) // 2
    reductions = [Reduction(side, t0_ref, sum0_ref, scratch[:count]), Reduction(side, t1_ref, sum1_ref, scratch[count:])]
    run_stages(reductions, (0, 2, 6, 7))
    by_a = dot_nt(by_gate_ref[...], wg_ref[...]).astype(BF16).astype(F32)
    by_a += dot_nt(by_up_ref[...], wu_ref[...]).astype(BF16).astype(F32)
    by_a = by_a.astype(BF16).astype(F32)
    out_ref[...] = by_h_ref[...] + backward_of_norm(h_ref[...], by_a).astype(BF16)
    last_stage(reductions)


MESH = pl.DeviceIdType.MESH


class Gather:
    STAGES = 5

    @staticmethod
    def scratch(shards):
        return [
            *(pltpu.VMEM(t.shape[1:], BF16) for t in shards),
            pltpu.SemaphoreType.DMA((4, 12)),
            pltpu.SemaphoreType.DMA((4, 12)),
            pltpu.SemaphoreType.DMA((6,)),
        ]

    def __init__(self, side, layer, shards, outs, scratch):
        self.side, self.layer, self.shards, self.outs, self.held = side, layer, shards, outs, scratch[:3]
        self.send_sem, self.recv_sem, self.own_sem = scratch[3:]
        me = lax.axis_index("dp")
        self.at = me // side, me % side
        half = shards[2].shape[1] // 2
        self.items = [
            (shards[0], outs[0], 0, 0, shards[0].shape[1]),
            (shards[1], outs[1], 1, 0, shards[1].shape[1]),
            (shards[2], outs[2], 0, 0, half),
            (shards[2], outs[2], 1, half, half),
        ]

    def beside(self, axis, by):
        x, y = self.at
        side = self.side
        return ((x + by) % side) * side + y if axis == 0 else x * side + (y + by) % side

    def part(self, item, which):
        _, _, _, start, rows = self.items[item]
        cut = cut_of(rows)
        return pl.ds(start, cut) if which == 0 else pl.ds(start + cut, rows - cut)

    def slot(self, item, by, which):
        x, y = self.at
        _, out, axis, _, _ = self.items[item]
        at = ((x + by) % self.side, y) if axis == 0 else (x, (y + by) % self.side)
        return out.at[at[0], at[1], self.part(item, which)]

    def line(self, item, by, which):
        x, y = self.at
        _, out, axis, _, _ = self.items[item]
        if axis == 0:
            return out.at[:, (y + by) % self.side, self.part(item, which)]
        return out.at[(x + by) % self.side, :, self.part(item, which)]

    def copy(self, item, number):
        shard, _, first, _, _ = self.items[item]
        back = self.side - 1
        by, which = ((1, 0), (back, 1), (1, 1), (back, 0), (1, 0), (back, 1), (1, 0), (back, 1), (1, 1), (back, 0), (1, 0), (back, 1))[number]
        behind = -by % self.side
        if number < 4:
            src, dst = shard.at[self.layer, self.part(item, which)], self.slot(item, 0, which)
        elif number < 6:
            src = dst = self.slot(item, behind, which)
        elif number < 10:
            src = dst = self.line(item, 0, which)
        else:
            src = dst = self.line(item, behind, which)
        return pltpu.make_async_remote_copy(
            src_ref=src,
            dst_ref=dst,
            send_sem=self.send_sem.at[item, number],
            recv_sem=self.recv_sem.at[item, number],
            device_id={"dp": self.beside(first if number < 6 else 1 - first, by)},
            device_id_type=MESH,
        )

    def own(self, number):
        return pltpu.make_async_copy(self.shards[number].at[self.layer], self.held[number], self.own_sem.at[number])

    def placed(self, number):
        x, y = self.at
        return pltpu.make_async_copy(self.held[number], self.outs[number].at[x, y], self.own_sem.at[3 + number])

    def stage(self, number):
        items = range(len(self.items))
        if number == 0:
            barrier = pltpu.get_barrier_semaphore()
            for axis in range(2):
                for by in (1, self.side - 1):
                    pl.semaphore_signal(barrier, inc=1, device_id={"dp": self.beside(axis, by)}, device_id_type=MESH)
            pl.semaphore_wait(barrier, 4)
            for k in range(3):
                self.own(k).start()
        if number == 1:
            for k in range(3):
                self.own(k).wait()
                self.placed(k).start()
        if number == 2:
            for k in range(3):
                self.placed(k).wait()
        waits, starts = (((), range(4)), ((0, 1), (4, 5)), ((2, 3, 4, 5), range(6, 10)), ((6, 7), (10, 11)), ((8, 9, 10, 11), ()))[number]
        for pair in range(0, max(len(waits), len(starts)), 2):
            for item in items:
                for k in waits[pair : pair + 2]:
                    self.copy(item, k).wait_recv()
                if number in (1, 3):
                    for k in starts:
                        self.copy(item, k).start()
        if number in (0, 2):
            for pair in range(0, len(starts), 2):
                for item in items:
                    for k in starts[pair : pair + 2]:
                        self.copy(item, k).start()
        if number == 4:
            for item in items:
                for k in range(12):
                    self.copy(item, k).wait_send()


def gather_kernel(side, *refs):
    gather = Gather(side, 0, refs[:3], refs[3:6], refs[6:])
    for number in range(Gather.STAGES):
        gather.stage(number)


def gathered(side, shards):
    return [((side, side, *t.shape[1:]), BF16) for t in shards]


def gather_first(side, *shards):
    return pl.pallas_call(
        functools.partial(gather_kernel, side),
        name="gather",
        in_specs=[ANY] * 3,
        out_specs=[ANY] * 3,
        out_shape=[jax.ShapeDtypeStruct(s, t) for s, t in gathered(side, shards)],
        scratch_shapes=Gather.scratch(shards),
        compiler_params=pltpu.CompilerParams(collective_id=0, has_side_effects=True, vmem_limit_bytes=VMEM),
        cost_estimate=pl.CostEstimate(flops=60_000_000_000, bytes_accessed=60_000_000, transcendentals=0),
    )(*shards)


ANY = pl.BlockSpec(memory_space=pl.ANY)


def tiled(n):
    return pl.BlockSpec((TILE, n), lambda i: (i, 0))


def whole(*shape):
    return pl.BlockSpec(shape, lambda i: (0,) * len(shape), pipeline_mode=pl.Buffered(1))


def call(kernel, name, grid, in_specs, out_specs, out_shape, scratch, matmuls, sizes, collective=None):
    tokens, d, ff = sizes
    return pl.pallas_call(
        kernel,
        name=name,
        grid=(grid,),
        in_specs=in_specs,
        out_specs=out_specs,
        out_shape=[jax.ShapeDtypeStruct(s, t) for s, t in out_shape],
        scratch_shapes=scratch,
        compiler_params=pltpu.CompilerParams(
            dimension_semantics=("arbitrary",), vmem_limit_bytes=VMEM, collective_id=collective, has_side_effects=collective is not None
        ),
        cost_estimate=pl.CostEstimate(flops=matmuls * 2 * tokens * d * ff, bytes_accessed=matmuls * 20_000_000, transcendentals=0),
    )


def solution(mesh):
    def step(x, dy, w_gate, w_up, w_down):
        shape, x, dy = x.shape, x[0], dy[0]
        tokens, d = x.shape
        ff = w_gate.shape[2]
        sizes, steps = (tokens, d, ff), tokens // TILE
        devices = mesh.shape["dp"]
        side = math.isqrt(devices)
        shards = w_gate, w_up, w_down
        first = [t.reshape(-1, t.shape[-1]) for t in gather_first(side, *shards)]

        weights = [whole(d, ff), whole(d, ff), whole(ff, d)]
        hidden, states = ((tokens, ff), BF16), ((tokens, d), BF16)
        gate, up, h, *second = call(
            functools.partial(forward_kernel, side), "fwd", steps,
            [tiled(d), *weights, ANY, ANY, ANY], [tiled(ff), tiled(ff), tiled(d), ANY, ANY, ANY],
            [((tokens, ff), F32), ((tokens, ff), F32), states, *gathered(side, shards)], Gather.scratch(shards), 3, sizes, 7,
        )(x, *first, *shards)
        second = [t.reshape(-1, t.shape[-1]) for t in second]
        wg, wu, wd = zip(first, second, strict=True)

        backward_out = dict(
            out_specs=[tiled(ff), tiled(ff), whole(ff, d)],
            out_shape=[hidden, hidden, ((ff, d), BF16)],
            scratch=[pltpu.VMEM((d, ff), F32)],
            sizes=sizes,
        )

        def reducing(t):
            rows, columns = t.shape[0] // devices, t.shape[1]
            return (
                t.reshape(side, side, rows, columns),
                whole(rows, columns),
                ((rows, columns), BF16),
                Reduction.scratch(side, rows, columns),
            )

        def by_weight(h, by_gate, by_up, t, name, collective):
            t, spec, shape, scratch = reducing(t)
            half = ff // PIECE
            early, late = (lambda i: (0, jnp.minimum(i, half - 1))), (lambda i: (0, jnp.maximum(i - half, 0)))
            return call(
                functools.partial(weight_kernel, side), name, 2 * half,
                [whole(tokens, d), pl.BlockSpec((tokens, PIECE), early), pl.BlockSpec((tokens, PIECE), late), ANY],
                [pl.BlockSpec((d, PIECE), early), pl.BlockSpec((d, PIECE), late), spec],
                [((d, ff), BF16), ((d, ff), BF16), shape], [pltpu.VMEM((d, tokens), BF16), *scratch], 2, sizes, collective,
            )(h, by_gate, by_up, t)

        def by_input(h, by_h, by_gate, by_up, n, terms, collective):
            terms, specs, shapes, scratch = zip(*map(reducing, terms), strict=True)
            return call(
                functools.partial(input_kernel, side), f"input{n}", steps,
                [tiled(d), tiled(d), tiled(ff), tiled(ff), *weights[:2], ANY, ANY],
                [tiled(d), *specs], [states, *shapes], [*scratch[0], *scratch[1]], 2, sizes, collective,
            )(h, by_h, by_gate, by_up, wg[n], wu[n], *terms)

        by_gate, by_up, by_wd = call(
            turn_kernel, "turn", steps, [tiled(d), tiled(d), *weights], matmuls=4, **backward_out
        )(h, dy, wg[1], wu[1], wd[1])
        by_wg, by_wu, down1 = by_weight(h, by_gate, by_up, by_wd, "weights1", 1)
        by_h, gate1, up1 = by_input(h, dy, by_gate, by_up, 1, (by_wg, by_wu), 2)

        by_gate, by_up, by_wd = call(
            back_kernel, "back", steps, [tiled(ff), tiled(ff), tiled(d), weights[2]], matmuls=2, **backward_out
        )(gate, up, by_h, wd[0])
        by_wg, by_wu, down0 = by_weight(x, by_gate, by_up, by_wd, "weights0", 3)
        by_x, gate0, up0 = by_input(x, by_h, by_gate, by_up, 0, (by_wg, by_wu), 4)
        return by_x.reshape(shape), jnp.stack([gate0, gate1]), jnp.stack([up0, up1]), jnp.stack([down0, down1])

    sequences, rows, gradients = P(("rep", "dp"), None, None), P(None, "dp", None), P("rep", "dp", None)
    return jax.shard_map(
        step,
        mesh=mesh,
        in_specs=(sequences, sequences, rows, rows, rows),
        out_specs=(sequences, gradients, gradients, gradients),
        check_vma=False,
    )
```
